512 devices in a mesh: lat: 32 (over z, x_hi), lon: 16 (over y, x_lo, core).
Axes of the slice: x: 4 (x_hi: 2, x_lo: 2; x = x_hi * 2 + x_lo), y: 4, z: 16, core: 2. Of those that a mesh axis runs over, the one named last changes fastest.
Arguments:
- fields: float32 [8, 32, 512, 2048], P(None, None, 'lat', 'lon'), may hold values from -6 to 6
- ocean_mask: int32 [512, 16], replicated, may hold values from 0 to 1, as said below
- scale_table: float32 [16], replicated, may hold values from 0.5 to 4
- offset_table: float32 [16], replicated, may hold values from -4 to 4
- scale_index: int32 [8], replicated, may hold values from 0 to 15
- offset_index: int32 [8], replicated, may hold values from 0 to 15
Outputs:
- history: float32 [8, 32, 512, 2048], P(None, 'lat', 'lon')
- record_range: float32 [2, 8, 32], P(None, None, 'lat')
The draws below stay inside these ranges and needn't reach their ends.
Inputs may be any that keep to these rules, and one draw needn't show every extreme that they name: `ocean_mask`: each device's block of 16 rows and 128 longitudes holds at least half of 12 (rounded down, and never fewer than one) and at most 12 ocean strips; some block holds exactly 12.
All inputs are finite; a program needn't handle non-finite values.
Results may differ from the reference program's by a relative error of at most 0.00007.
Values sent between devices are 32-bit elements; how exact they have to be, the bound alone decides.
A program may use at most 64 MiB of HBM per device.

```python
import math
import jax
import jax.numpy as jnp

FIELDS = 8
TABLE = 16
LAT_DEV = 16
LON_DEV = 128
STRIP = 128
LEVELS = 32
NLAT = 512
NLON = 2048
NSTRIP = 16
MAX_LIVE = 12


def draw_ocean_mask(key, part):
    strips_row = LON_DEV // STRIP
    per_block = LAT_DEV * strips_row
    blocks_lat = NLAT // LAT_DEV
    blocks_lon = NSTRIP // strips_row
    total_blocks = blocks_lat * blocks_lon
    count_key = jax.random.fold_in(key, 11)
    full_key = jax.random.fold_in(key, 12)
    score_key = jax.random.fold_in(key, 13)
    fewest = max(1, MAX_LIVE // 2)
    counts = jax.random.randint(count_key, (total_blocks,), fewest, MAX_LIVE + 1)
    full_block = jax.random.randint(full_key, (), 0, total_blocks)
    counts = jnp.where(jnp.arange(total_blocks) == full_block, MAX_LIVE, counts)
    scores = jax.random.randint(score_key, (total_blocks, per_block), 0, 1 << 20) * per_block
    scores = scores + jnp.arange(per_block)[None, :]
    ranks = jnp.argsort(jnp.argsort(scores, axis=1), axis=1)
    ocean = (ranks < counts[:, None]).astype(jnp.int32)
    ocean = ocean.reshape(blocks_lat, blocks_lon, LAT_DEV, strips_row).transpose(0, 2, 1, 3)
    return ocean.reshape(NLAT, NSTRIP)


def with_ends(entries, own_key, smallest, top_value):
    dims = entries.shape
    place = [jax.random.randint(jax.random.fold_in(own_key, axis), (), 0, dims[axis]) for axis in range(len(dims))]
    entries = entries.at[tuple(place)].set(smallest)
    longest = dims.index(max(dims))
    place[longest] = (place[longest] + 1) % dims[longest]
    return entries.at[tuple(place)].set(top_value)


def levels(own_key, extent, split, low, largest):
    loudness, own = 1.0, jax.random.fold_in(own_key, 6)
    for dim, blocks in split:
        heights = jnp.exp(jax.random.uniform(jax.random.fold_in(own, dim), (blocks,), jnp.float32, low / len(split), largest / len(split)))
        loudness = loudness * jnp.repeat(heights, extent[dim] // blocks).reshape([-1 if axis == dim else 1 for axis in range(len(extent))])
    return loudness


def bell_draw(own_key, dims, scale, limit, split=(), held_as=jnp.bfloat16):
    drawn = jax.random.normal(own_key, dims, jnp.float32) * scale
    if len(split) > 0:
        drawn = levels(own_key, dims, split, -0.22, 0.18) * drawn
    return jnp.clip(drawn, min=-limit, max=limit).astype(held_as)


def setup_inputs(seed: int = 0) -> dict:
    splits = jax.random.split(jax.random.key(seed), 7)
    return {
        "fields": bell_draw(splits[0], (FIELDS, LEVELS, NLAT, NLON), 1.0, 6.0, ((2, 32), (3, 16)), jnp.float32),
        "ocean_mask": draw_ocean_mask(jax.random.fold_in(splits[6], 71), 0),
        "scale_table": jnp.clip(jnp.exp(jax.random.uniform(splits[2], (TABLE,), jnp.float32, math.log(0.5), math.log(4.0))), 0.5, 4.0),
        "offset_table": bell_draw(splits[3], (TABLE,), 1.0, 4.0, (), jnp.float32),
        "scale_index": with_ends(jax.random.randint(splits[4], (FIELDS,), 0, TABLE), jax.random.fold_in(splits[4], 1), 0, TABLE - 1).astype(jnp.int32),
        "offset_index": with_ends(jax.random.randint(splits[5], (FIELDS,), 0, TABLE), jax.random.fold_in(splits[5], 1), 0, TABLE - 1).astype(jnp.int32),
    }


def reference(fields, ocean_mask, scale_table, offset_table, scale_index, offset_index):
    scales = scale_table[scale_index].astype(jnp.float32)
    offsets = offset_table[offset_index].astype(jnp.float32)
    ocean_cells = jnp.repeat(ocean_mask, STRIP, axis=1) > 0
    packed = (fields - offsets[:, None, None, None]) * scales[:, None, None, None]
    history = jnp.where(ocean_cells[None, None], packed, jnp.zeros_like(packed))
    highest = jnp.max(jnp.where(ocean_cells[None, None], packed, -jnp.inf), axis=(2, 3))
    lowest = jnp.min(jnp.where(ocean_cells[None, None], packed, jnp.inf), axis=(2, 3))
    return history, jnp.stack([highest, lowest])
```

```python
import functools

import jax
import jax.numpy as jnp
from jax import lax
from jax.experimental import pallas as pl
from jax.experimental.pallas import tpu as pltpu
from jax.sharding import PartitionSpec as P

MESH = pl.DeviceIdType.MESH
FIELDS = 8
LEVELS = 32
ROWS = 16
LANES = 128
SLOTS = 12
PLANES = 16
LONS = 16
SENDERS = 32
FIELD_STRIDE = LEVELS * ROWS + 8
OUT_STRIDE = 2 * ROWS * LONS
STEPS = PLANES // 2
LAG = 2
STRIDE = 3

def remote(src, dst, send_sem, recv_sem, device):
    return pltpu.make_async_remote_copy(
        src_ref=src, dst_ref=dst, send_sem=send_sem, recv_sem=recv_sem,
        device_id=device, device_id_type=MESH,
    )


def kernel(
    scale_hbm, offset_hbm, scale_index_hbm, offset_index_hbm, fields, mask,
    out, range_out,
    scale_table, offset_table, scale_index, offset_index, staged, own_mask, slab_mask, packed, passing, arrived, block, spread_out,
    stat, stat_in, part, part_in, total, range_in,
    load_sem, mask_sem, table_sem, column_send, column_recv,
    send_sem, recv_sem, stat_send, stat_recv, part_send, part_recv, range_send, range_recv, out_sem,
):
    lat = lax.axis_index("lat")
    lon = lax.axis_index("lon")
    plane = lat // 2
    half = lat % 2
    me = half * LONS + lon
    barrier = pltpu.get_barrier_semaphore()

    def at_plane(offset):
        return (lax.rem(plane + offset + PLANES, PLANES) * 2 + half, lon)

    def in_plane(i):
        return (plane * 2 + i // LONS, lax.rem(i, LONS))

    def signal_column(k, carry):
        pl.semaphore_signal(barrier, inc=1, device_id=at_plane(k), device_id_type=MESH)
        return carry

    def signal_plane(k, carry):
        pl.semaphore_signal(
            barrier, inc=1, device_id=in_plane(lax.rem(me + k, SENDERS)), device_id_type=MESH
        )
        return carry

    lax.fori_loop(1, PLANES, signal_column, 0)
    lax.fori_loop(1, SENDERS, signal_plane, 0)

    own_column = pl.multiple_of((lat // 8) * LANES, LANES)
    slab_column = pl.multiple_of((lon // 4) * LANES, LANES)
    own_load = pltpu.make_async_copy(
        mask.at[:, pl.ds(own_column, LANES)], own_mask, mask_sem.at[0]
    )
    slab_load = pltpu.make_async_copy(
        mask.at[:, pl.ds(slab_column, LANES)], slab_mask, mask_sem.at[1]
    )
    own_load.start()
    slab_load.start()
    table_loads = [
        pltpu.make_async_copy(src, dst, table_sem.at[i])
        for i, (src, dst) in enumerate((
            (scale_hbm, scale_table), (offset_hbm, offset_table),
            (scale_index_hbm, scale_index), (offset_index_hbm, offset_index),
        ))
    ]
    for load in table_loads:
        load.start()
    loads = [
        pltpu.make_async_copy(
            fields.at[f], staged.at[pl.ds(f * FIELD_STRIDE, LEVELS * ROWS)], load_sem.at[f]
        )
        for f in range(FIELDS)
    ]
    for load in loads:
        load.start()

    for load in table_loads:
        load.wait()
    field_row = lax.broadcasted_iota(jnp.int32, (FIELDS, LANES), 0)
    lane = lax.broadcasted_iota(jnp.int32, (FIELDS, LANES), 1)
    scales = jnp.zeros((FIELDS, LANES), jnp.float32)
    offsets = jnp.zeros((FIELDS, LANES), jnp.float32)
    for f in range(FIELDS):
        scales = jnp.where(field_row == f, scale_table[scale_index[f]], scales)
        offsets = jnp.where(field_row == f, offset_table[offset_index[f]], offsets)

    own_load.wait()
    first = (lat % 8) * ROWS
    live = [own_mask[lon, first + s] for s in range(ROWS)]
    chosen = [jnp.int32(0)] * SLOTS
    count = jnp.int32(0)
    for s in range(ROWS):
        for k in range(SLOTS):
            if k <= s:
                chosen[k] = jnp.where((live[s] > 0) & (count == k), s, chosen[k])
        count = count + live[s]
    for k in range(1, SLOTS):
        chosen[k] = jnp.where(k < count, chosen[k], chosen[0])

    for load in loads:
        load.wait()

    def pack(level, carry):
        base = level * ROWS
        highest = None
        lowest = None
        for k in range(SLOTS):
            rows = staged[pl.ds(base + chosen[k], FIELDS, stride=FIELD_STRIDE), :]
            value = (rows - offsets) * scales
            packed[level, k] = value
            highest = value if k == 0 else jnp.maximum(highest, value)
            lowest = value if k == 0 else jnp.minimum(lowest, value)
        high = jnp.max(highest, axis=1, keepdims=True)
        low = jnp.max(-lowest, axis=1, keepdims=True)
        spread = jnp.where(
            lane == field_row, high, jnp.where(lane == field_row + FIELDS, low, -jnp.inf)
        )
        stat[level] = jnp.max(spread, axis=0, keepdims=True)
        return carry

    lax.fori_loop(0, LEVELS, pack, 0)

    pl.semaphore_wait(barrier, PLANES + SENDERS - 2)

    turn = lon // 2

    def distance(step):
        return 1 + lax.rem(STRIDE * step + turn, STEPS)

    def column_copy(step, sign):
        offset = distance(step) * (1 - 2 * sign)
        level = pl.multiple_of(lax.rem(plane + offset + PLANES, PLANES) * 2, 2)
        return remote(
            packed.at[pl.ds(level, 2)], passing.at[step, sign],
            column_send.at[step, sign], column_recv.at[step, sign], at_plane(offset),
        )

    def both_signs(step, act):
        act(0)

        @pl.when(distance(step) < STEPS)
        def _():
            act(1)

    def hand_on(source, slot, origin):
        for h in range(2):
            mine = (origin == lon) & (half == h)

            @pl.when(jnp.logical_not(mine))
            def _():
                remote(
                    source(h), arrived.at[me], send_sem.at[slot, h], recv_sem.at[me],
                    (plane * 2 + h, origin),
                ).start()

            @pl.when(mine)
            def _():
                for k in range(SLOTS):
                    arrived[me, k] = source(h)[k]

    def handed_on(source, slot, origin):
        for h in range(2):
            @pl.when(jnp.logical_not((origin == lon) & (half == h)))
            def _():
                remote(
                    source(h), arrived.at[0], send_sem.at[slot, h], recv_sem.at[0], (lat, lon)
                ).wait_send()

    def send_stat(k, carry):
        level = lax.rem(me + k, SENDERS)
        remote(
            stat.at[level], stat_in.at[me], stat_send.at[level], stat_recv.at[me], in_plane(level)
        ).start()
        return carry

    lax.fori_loop(1, SENDERS, send_stat, 0)
    stat_in[me] = stat[me]

    def start_column(step, carry):
        both_signs(step, lambda sign: column_copy(step, sign).start())
        return carry

    lax.fori_loop(0, STEPS, start_column, 0)
    hand_on(lambda h: packed.at[plane * 2 + h], 2 * STEPS, plane)

    def take_stat(k, best):
        i = lax.rem(me + k, SENDERS)
        remote(stat.at[0], stat_in.at[i], stat_send.at[i], stat_recv.at[i], (lat, lon)).wait_recv()
        return jnp.maximum(best, stat_in[i])

    best = lax.fori_loop(1, SENDERS, take_stat, stat_in[me])
    part[...] = best
    for k in range(1, PLANES):
        remote(part, part_in.at[k], part_send.at[k], part_recv.at[k], at_plane(k)).start()

    slab_load.wait()
    slab_first = (lon % 4) * 2 * ROWS

    def unpack(i):
        h = i // LONS
        q = lax.rem(i, LONS)

        @pl.when(i != me)
        def _():
            remote(
                packed.at[0], arrived.at[i], send_sem.at[0, 0], recv_sem.at[i], (lat, lon)
            ).wait_recv()

        for k in range(SLOTS):
            block[k] = arrived[i, k]
        rank = jnp.int32(0)
        for s in range(ROWS):
            wet = slab_mask[q, slab_first + h * ROWS + s]
            value = block[jnp.minimum(rank, SLOTS - 1)]
            rank = rank + wet
            row = (h * 2 + s // 8) * (LONS * 8) + q * 8 + s % 8
            spread_out[pl.ds(row, FIELDS, stride=OUT_STRIDE), :] = jnp.where(wet > 0, value, 0.0)

    away = lax.rem(plane - lon + PLANES, PLANES)
    away = jnp.where(away > STEPS, PLANES - away, away)

    def unpack_step(step):
        column = lax.rem(away - 1 - STRIDE * step + 8 * STEPS, STEPS) * 2
        for h in range(2):
            for c in range(2):
                unpack(h * LONS + column + c)

    def relay(step, carry):
        def pass_on(sign):
            column_copy(step, sign).wait_recv()
            origin = lax.rem(plane - distance(step) * (1 - 2 * sign) + PLANES, PLANES)
            hand_on(lambda h: passing.at[step, sign, h], 2 * step + sign, origin)

        both_signs(step, pass_on)

        @pl.when(step >= LAG)
        def _():
            unpack_step(step - LAG)
        return carry

    lax.fori_loop(0, STEPS, relay, 0)

    best = part[...]
    for k in range(1, PLANES):
        remote(part, part_in.at[k], part_send.at[k], part_recv.at[k], (lat, lon)).wait_recv()
        best = jnp.maximum(best, part_in[k])
    total[...] = best
    tells = me // 2 == plane

    def range_copy(q):
        return remote(
            total, range_in, range_send.at[q], range_recv, (plane * 2 + lax.rem(me, 2), q)
        )

    def told_self(q):
        return (q == lon) & (lax.rem(me, 2) == half)

    def tell(q, carry):
        @pl.when(tells & jnp.logical_not(told_self(q)))
        def _():
            range_copy(q).start()

        @pl.when(tells & told_self(q))
        def _():
            range_in[...] = total[...]
        return carry

    lax.fori_loop(0, LONS, tell, 0)

    def unpack_rest(step, carry):
        unpack_step(step)
        return carry

    lax.fori_loop(STEPS - LAG, STEPS, unpack_rest, 0)
    stores = [
        pltpu.make_async_copy(
            spread_out.at[pl.ds(f * OUT_STRIDE, OUT_STRIDE)], out.at[f], out_sem.at[f]
        )
        for f in range(FIELDS)
    ]
    for store in stores:
        store.start()

    @pl.when(jnp.logical_not((lat == me)))
    def _():
        remote(total, range_in, range_send.at[0], range_recv, (lat, lon)).wait_recv()

    range_out[...] = range_in[...]

    def told(q, carry):
        @pl.when(tells & jnp.logical_not(told_self(q)))
        def _():
            range_copy(q).wait_send()
        return carry

    lax.fori_loop(0, LONS, told, 0)

    def drain_stat(k, carry):
        level = lax.rem(me + k, SENDERS)
        remote(
            stat.at[level], stat_in.at[0], stat_send.at[level], stat_recv.at[0], (lat, lon)
        ).wait_send()
        return carry

    lax.fori_loop(1, SENDERS, drain_stat, 0)

    def drain(step, carry):
        def one(sign):
            column_copy(step, sign).wait_send()
            origin = lax.rem(plane - distance(step) * (1 - 2 * sign) + PLANES, PLANES)
            handed_on(lambda h: passing.at[step, sign, h], 2 * step + sign, origin)

        both_signs(step, one)
        return carry

    lax.fori_loop(0, STEPS, drain, 0)
    handed_on(lambda h: packed.at[plane * 2 + h], 2 * STEPS, plane)
    for k in range(1, PLANES):
        remote(part, part_in.at[k], part_send.at[k], part_recv.at[k], (lat, lon)).wait_send()
    for store in stores:
        store.wait()


def per_device(fields, ocean_mask, scale_table, offset_table, scale_index, offset_index):
    vmem = pl.BlockSpec(memory_space=pltpu.VMEM)
    hbm = pl.BlockSpec(memory_space=pltpu.HBM)
    dma = pltpu.SemaphoreType.DMA
    out, best = pl.pallas_call(
        kernel,
        name="exchange",
        out_shape=(
            jax.ShapeDtypeStruct((FIELDS, OUT_STRIDE, LANES), jnp.float32),
            jax.ShapeDtypeStruct((1, LANES), jnp.float32),
        ),
        in_specs=[hbm] * 6,
        out_specs=(hbm, vmem),
        scratch_shapes=[
            pltpu.SMEM((16,), jnp.float32), pltpu.SMEM((16,), jnp.float32),
            pltpu.SMEM((FIELDS,), jnp.int32), pltpu.SMEM((FIELDS,), jnp.int32),
            pltpu.VMEM((FIELDS * FIELD_STRIDE, LANES), jnp.float32),
            pltpu.SMEM((LONS, LANES), jnp.int32),
            pltpu.SMEM((LONS, LANES), jnp.int32),
            pltpu.VMEM((LEVELS, SLOTS, FIELDS, LANES), jnp.float32),
            pltpu.VMEM((STEPS, 2, 2, SLOTS, FIELDS, LANES), jnp.float32),
            pltpu.VMEM((SENDERS, SLOTS, FIELDS, LANES), jnp.float32),
            pltpu.VMEM((SLOTS, FIELDS, LANES), jnp.float32),
            pltpu.VMEM((FIELDS * OUT_STRIDE, LANES), jnp.float32),
            pltpu.VMEM((LEVELS, 1, LANES), jnp.float32),
            pltpu.VMEM((SENDERS, 1, LANES), jnp.float32),
            pltpu.VMEM((1, LANES), jnp.float32),
            pltpu.VMEM((PLANES, 1, LANES), jnp.float32),
            pltpu.VMEM((1, LANES), jnp.float32),
            pltpu.VMEM((1, LANES), jnp.float32),
            dma((FIELDS,)), dma((2,)), dma((4,)),
            dma((STEPS, 2)), dma((STEPS, 2)), dma((2 * STEPS + 1, 2)), dma((SENDERS,)),
            dma((LEVELS,)), dma((SENDERS,)), dma((PLANES,)), dma((PLANES,)),
            dma((LONS,)), dma, dma((FIELDS,)),
        ],
        compiler_params=pltpu.CompilerParams(
            collective_id=0, has_side_effects=True, vmem_limit_bytes=65472 * 1024
        ),
    )(
        scale_table, offset_table, scale_index, offset_index,
        fields.reshape(FIELDS, LEVELS * ROWS, LANES), ocean_mask.T,
    )
    history = out.reshape(FIELDS, 4, LONS, 8, LANES).transpose(0, 1, 3, 2, 4)
    history = history.reshape(FIELDS, 1, 2 * ROWS, LONS * LANES)
    record_range = jnp.stack([best[0, :FIELDS], -best[0, FIELDS:2 * FIELDS]])[:, :, None]
    return history, record_range


def solution(mesh):
    return jax.shard_map(
        per_device,
        mesh=mesh,
        in_specs=(P(None, None, "lat", "lon"), P(), P(), P(), P(), P()),
        out_specs=(P(None, "lat", "lon", None), P(None, None, "lat")),
        check_vma=False,
    )
```

```python
import functools

import jax
import jax.numpy as jnp
from jax import lax
from jax.experimental import pallas as pl
from jax.experimental.pallas import tpu as pltpu
from jax.sharding import PartitionSpec as P

MESH = pl.DeviceIdType.MESH
FIELDS = 8
LEVELS = 32
ROWS = 16
LANES = 128
SLOTS = 12
PLANES = 16
LONS = 16
SENDERS = 32
FIELD_STRIDE = LEVELS * ROWS + 8
OUT_STRIDE = 2 * ROWS * LONS
STEPS = PLANES // 2
LAG = 2
EARLY = 4
TELL = 6
STRIDE = 3

def remote(src, dst, send_sem, recv_sem, device):
    return pltpu.make_async_remote_copy(
        src_ref=src, dst_ref=dst, send_sem=send_sem, recv_sem=recv_sem,
        device_id=device, device_id_type=MESH,
    )


def kernel(
    scale_hbm, offset_hbm, scale_index_hbm, offset_index_hbm, fields, mask,
    out, range_out,
    scale_table, offset_table, scale_index, offset_index, staged, own_mask, slab_mask, packed, passing, arrived, block, spread_out, highs, lows,
    stat, stat_in, part, part_in, total, range_in,
    load_sem, mask_sem, table_sem, column_send, column_recv,
    send_sem, recv_sem, stat_send, stat_recv, part_send, part_recv, range_send, range_recv, out_sem,
):
    lat = lax.axis_index("lat")
    lon = lax.axis_index("lon")
    plane = lat // 2
    half = lat % 2
    me = half * LONS + lon
    barrier = pltpu.get_barrier_semaphore()

    def at_plane(offset):
        return (lax.rem(plane + offset + PLANES, PLANES) * 2 + half, lon)

    def in_plane(i):
        return (plane * 2 + i // LONS, lax.rem(i, LONS))

    def signal_column(k, carry):
        pl.semaphore_signal(barrier, inc=1, device_id=at_plane(k), device_id_type=MESH)
        return carry

    def signal_plane(k, carry):
        pl.semaphore_signal(
            barrier, inc=1, device_id=in_plane(lax.rem(me + k, SENDERS)), device_id_type=MESH
        )
        return carry

    lax.fori_loop(1, PLANES, signal_column, 0)
    lax.fori_loop(1, SENDERS, signal_plane, 0)

    own_column = pl.multiple_of((lat // 8) * LANES, LANES)
    slab_column = pl.multiple_of((lon // 4) * LANES, LANES)
    own_load = pltpu.make_async_copy(
        mask.at[:, pl.ds(own_column, LANES)], own_mask, mask_sem.at[0]
    )
    slab_load = pltpu.make_async_copy(
        mask.at[:, pl.ds(slab_column, LANES)], slab_mask, mask_sem.at[1]
    )
    own_load.start()
    slab_load.start()
    table_loads = [
        pltpu.make_async_copy(src, dst, table_sem.at[i])
        for i, (src, dst) in enumerate((
            (scale_hbm, scale_table), (offset_hbm, offset_table),
            (scale_index_hbm, scale_index), (offset_index_hbm, offset_index),
        ))
    ]
    for load in table_loads:
        load.start()
    loads = [
        pltpu.make_async_copy(
            fields.at[f], staged.at[pl.ds(f * FIELD_STRIDE, LEVELS * ROWS)], load_sem.at[f]
        )
        for f in range(FIELDS)
    ]
    for load in loads:
        load.start()

    for load in table_loads:
        load.wait()
    field_row = lax.broadcasted_iota(jnp.int32, (FIELDS, LANES), 0)
    lane = lax.broadcasted_iota(jnp.int32, (FIELDS, LANES), 1)
    scales = jnp.zeros((FIELDS, LANES), jnp.float32)
    offsets = jnp.zeros((FIELDS, LANES), jnp.float32)
    for f in range(FIELDS):
        scales = jnp.where(field_row == f, scale_table[scale_index[f]], scales)
        offsets = jnp.where(field_row == f, offset_table[offset_index[f]], offsets)

    own_load.wait()
    first = (lat % 8) * ROWS
    live = [own_mask[lon, first + s] for s in range(ROWS)]
    chosen = [jnp.int32(0)] * SLOTS
    count = jnp.int32(0)
    for s in range(ROWS):
        for k in range(SLOTS):
            if k <= s:
                chosen[k] = jnp.where((live[s] > 0) & (count == k), s, chosen[k])
        count = count + live[s]
    for k in range(1, SLOTS):
        chosen[k] = jnp.where(k < count, chosen[k], chosen[0])

    for load in loads:
        load.wait()

    def pack(turn_, carry):
        for u in range(4):
            level = turn_ * 4 + u
            highest = None
            lowest = None
            for k in range(SLOTS):
                rows = staged[pl.ds(level * ROWS + chosen[k], FIELDS, stride=FIELD_STRIDE), :]
                value = (rows - offsets) * scales
                packed[level, k] = value
                highest = value if k == 0 else jnp.maximum(highest, value)
                lowest = value if k == 0 else jnp.minimum(lowest, value)
            highs[level] = highest
            lows[level] = lowest
        return carry

    lax.fori_loop(0, LEVELS // 4, pack, 0)

    pl.semaphore_wait(barrier, PLANES + SENDERS - 2)

    turn = lon // 2

    def distance(step):
        return 1 + lax.rem(STRIDE * step + turn, STEPS)

    def column_copy(step, sign):
        offset = distance(step) * (1 - 2 * sign)
        level = pl.multiple_of(lax.rem(plane + offset + PLANES, PLANES) * 2, 2)
        return remote(
            packed.at[pl.ds(level, 2)], passing.at[step, sign],
            column_send.at[step, sign], column_recv.at[step, sign], at_plane(offset),
        )

    def both_signs(step, act):
        act(0)

        @pl.when(distance(step) < STEPS)
        def _():
            act(1)

    def hand_on(source, slot, origin):
        for h in range(2):
            mine = (origin == lon) & (half == h)

            @pl.when(jnp.logical_not(mine))
            def _():
                remote(
                    source(h), arrived.at[me], send_sem.at[slot, h], recv_sem.at[me],
                    (plane * 2 + h, origin),
                ).start()

            @pl.when(mine)
            def _():
                for k in range(SLOTS):
                    arrived[me, k] = source(h)[k]

    def handed_on(source, slot, origin):
        for h in range(2):
            @pl.when(jnp.logical_not((origin == lon) & (half == h)))
            def _():
                remote(
                    source(h), arrived.at[0], send_sem.at[slot, h], recv_sem.at[0], (lat, lon)
                ).wait_send()

    def start_column(step, carry):
        both_signs(step, lambda sign: column_copy(step, sign).start())
        return carry

    lax.fori_loop(0, EARLY, start_column, 0)

    def reduce_stat(turn_, carry):
        for u in range(4):
            level = turn_ * 4 + u
            high = jnp.max(highs[level], axis=1, keepdims=True)
            low = jnp.max(-lows[level], axis=1, keepdims=True)
            both = jnp.where(
                lane == field_row, high, jnp.where(lane == field_row + FIELDS, low, -jnp.inf)
            )
            stat[level] = jnp.max(both, axis=0, keepdims=True)
        return carry

    lax.fori_loop(0, LEVELS // 4, reduce_stat, 0)

    def send_stat(k, carry):
        level = lax.rem(me + k, SENDERS)
        remote(
            stat.at[level], stat_in.at[me], stat_send.at[level], stat_recv.at[me], in_plane(level)
        ).start()
        return carry

    lax.fori_loop(1, SENDERS, send_stat, 0)
    stat_in[me] = stat[me]
    hand_on(lambda h: packed.at[plane * 2 + h], 2 * STEPS, plane)

    def take_stat(k, best):
        i = lax.rem(me + k, SENDERS)
        remote(stat.at[0], stat_in.at[i], stat_send.at[i], stat_recv.at[i], (lat, lon)).wait_recv()
        return jnp.maximum(best, stat_in[i])

    best = lax.fori_loop(1, SENDERS, take_stat, stat_in[me])
    part[...] = best
    for k in range(1, PLANES):
        remote(part, part_in.at[k], part_send.at[k], part_recv.at[k], at_plane(k)).start()

    lax.fori_loop(EARLY, STEPS, start_column, 0)

    slab_load.wait()
    slab_first = (lon % 4) * 2 * ROWS

    def unpack(i):
        h = i // LONS
        q = lax.rem(i, LONS)

        @pl.when(i != me)
        def _():
            remote(
                packed.at[0], arrived.at[i], send_sem.at[0, 0], recv_sem.at[i], (lat, lon)
            ).wait_recv()

        for k in range(SLOTS):
            block[k] = arrived[i, k]
        rank = jnp.int32(0)
        for s in range(ROWS):
            wet = slab_mask[q, slab_first + h * ROWS + s]
            value = block[jnp.minimum(rank, SLOTS - 1)]
            rank = rank + wet
            row = (h * 2 + s // 8) * (LONS * 8) + q * 8 + s % 8
            spread_out[pl.ds(row, FIELDS, stride=OUT_STRIDE), :] = jnp.where(wet > 0, value, 0.0)

    away = lax.rem(plane - lon + PLANES, PLANES)
    away = jnp.where(away > STEPS, PLANES - away, away)

    def unpack_step(step):
        column = lax.rem(away - 1 - STRIDE * step + 8 * STEPS, STEPS) * 2
        for h in range(2):
            for c in range(2):
                unpack(h * LONS + column + c)

    def relay(step, carry):
        def pass_on(sign):
            column_copy(step, sign).wait_recv()
            origin = lax.rem(plane - distance(step) * (1 - 2 * sign) + PLANES, PLANES)
            hand_on(lambda h: passing.at[step, sign, h], 2 * step + sign, origin)

        both_signs(step, pass_on)

        @pl.when(step >= LAG)
        def _():
            unpack_step(step - LAG)
        return carry

    lax.fori_loop(0, TELL, relay, 0)

    best = part[...]
    for k in range(1, PLANES):
        remote(part, part_in.at[k], part_send.at[k], part_recv.at[k], (lat, lon)).wait_recv()
        best = jnp.maximum(best, part_in[k])
    total[...] = best
    tells = me // 2 == plane

    def range_copy(q):
        return remote(
            total, range_in, range_send.at[q], range_recv, (plane * 2 + lax.rem(me, 2), q)
        )

    def told_self(q):
        return (q == lon) & (lax.rem(me, 2) == half)

    def tell(q, carry):
        @pl.when(tells & jnp.logical_not(told_self(q)))
        def _():
            range_copy(q).start()

        @pl.when(tells & told_self(q))
        def _():
            range_in[...] = total[...]
        return carry

    lax.fori_loop(0, LONS, tell, 0)

    lax.fori_loop(TELL, STEPS, relay, 0)

    def unpack_rest(step, carry):
        unpack_step(step)
        return carry

    lax.fori_loop(STEPS - LAG, STEPS, unpack_rest, 0)
    stores = [
        pltpu.make_async_copy(
            spread_out.at[pl.ds(f * OUT_STRIDE, OUT_STRIDE)], out.at[f], out_sem.at[f]
        )
        for f in range(FIELDS)
    ]
    for store in stores:
        store.start()

    @pl.when(jnp.logical_not((lat == me)))
    def _():
        remote(total, range_in, range_send.at[0], range_recv, (lat, lon)).wait_recv()

    ends_row = range_in[...]
    range_out[0] = ends_row[:, :FIELDS]
    range_out[1] = -ends_row[:, FIELDS:2 * FIELDS]

    def told(q, carry):
        @pl.when(tells & jnp.logical_not(told_self(q)))
        def _():
            range_copy(q).wait_send()
        return carry

    lax.fori_loop(0, LONS, told, 0)

    def drain_stat(k, carry):
        level = lax.rem(me + k, SENDERS)
        remote(
            stat.at[level], stat_in.at[0], stat_send.at[level], stat_recv.at[0], (lat, lon)
        ).wait_send()
        return carry

    lax.fori_loop(1, SENDERS, drain_stat, 0)

    def drain(step, carry):
        def one(sign):
            column_copy(step, sign).wait_send()
            origin = lax.rem(plane - distance(step) * (1 - 2 * sign) + PLANES, PLANES)
            handed_on(lambda h: passing.at[step, sign, h], 2 * step + sign, origin)

        both_signs(step, one)
        return carry

    lax.fori_loop(0, STEPS, drain, 0)
    handed_on(lambda h: packed.at[plane * 2 + h], 2 * STEPS, plane)
    for k in range(1, PLANES):
        remote(part, part_in.at[k], part_send.at[k], part_recv.at[k], (lat, lon)).wait_send()
    for store in stores:
        store.wait()


def per_device(fields, ocean_mask, scale_table, offset_table, scale_index, offset_index):
    vmem = pl.BlockSpec(memory_space=pltpu.VMEM)
    hbm = pl.BlockSpec(memory_space=pltpu.HBM)
    dma = pltpu.SemaphoreType.DMA
    out, best = pl.pallas_call(
        kernel,
        name="exchange",
        out_shape=(
            jax.ShapeDtypeStruct((FIELDS, OUT_STRIDE, LANES), jnp.float32),
            jax.ShapeDtypeStruct((2, 1, FIELDS), jnp.float32),
        ),
        in_specs=[hbm] * 6,
        out_specs=(hbm, vmem),
        scratch_shapes=[
            pltpu.SMEM((16,), jnp.float32), pltpu.SMEM((16,), jnp.float32),
            pltpu.SMEM((FIELDS,), jnp.int32), pltpu.SMEM((FIELDS,), jnp.int32),
            pltpu.VMEM((FIELDS * FIELD_STRIDE, LANES), jnp.float32),
            pltpu.SMEM((LONS, LANES), jnp.int32),
            pltpu.SMEM((LONS, LANES), jnp.int32),
            pltpu.VMEM((LEVELS, SLOTS, FIELDS, LANES), jnp.float32),
            pltpu.VMEM((STEPS, 2, 2, SLOTS, FIELDS, LANES), jnp.float32),
            pltpu.VMEM((SENDERS, SLOTS, FIELDS, LANES), jnp.float32),
            pltpu.VMEM((SLOTS, FIELDS, LANES), jnp.float32),
            pltpu.VMEM((FIELDS * OUT_STRIDE, LANES), jnp.float32),
            pltpu.VMEM((LEVELS, FIELDS, LANES), jnp.float32),
            pltpu.VMEM((LEVELS, FIELDS, LANES), jnp.float32),
            pltpu.VMEM((LEVELS, 1, LANES), jnp.float32),
            pltpu.VMEM((SENDERS, 1, LANES), jnp.float32),
            pltpu.VMEM((1, LANES), jnp.float32),
            pltpu.VMEM((PLANES, 1, LANES), jnp.float32),
            pltpu.VMEM((1, LANES), jnp.float32),
            pltpu.VMEM((1, LANES), jnp.float32),
            dma((FIELDS,)), dma((2,)), dma((4,)),
            dma((STEPS, 2)), dma((STEPS, 2)), dma((2 * STEPS + 1, 2)), dma((SENDERS,)),
            dma((LEVELS,)), dma((SENDERS,)), dma((PLANES,)), dma((PLANES,)),
            dma((LONS,)), dma, dma((FIELDS,)),
        ],
        compiler_params=pltpu.CompilerParams(
            collective_id=0, has_side_effects=True, vmem_limit_bytes=65472 * 1024
        ),
    )(
        scale_table, offset_table, scale_index, offset_index,
        fields.reshape(FIELDS, LEVELS * ROWS, LANES), ocean_mask.T,
    )
    history = out.reshape(FIELDS, 4, LONS, 8, LANES).transpose(0, 1, 3, 2, 4)
    history = history.reshape(FIELDS, 1, 2 * ROWS, LONS * LANES)
    record_range = best.transpose(0, 2, 1)
    return history, record_range


def solution(mesh):
    return jax.shard_map(
        per_device,
        mesh=mesh,
        in_specs=(P(None, None, "lat", "lon"), P(), P(), P(), P(), P()),
        out_specs=(P(None, "lat", "lon", None), P(None, None, "lat")),
        check_vma=False,
    )
```
